128 devices in a mesh: data: 1, stage: 128 (over z, y, x, core).
Axes of the slice: x: 4, y: 4, z: 4, core: 2. Of those that a mesh axis runs over, the one named last changes fastest.
Arguments:
- x_enc: bfloat16 [128, 1024, 1024], P(('data', 'stage'))
- enc_len: int32 [128], P(('data', 'stage'))
- y: bfloat16 [128, 64, 1024], P(('data', 'stage'))
- enc_wqkv: bfloat16 [2, 1024, 3, 16, 128], replicated
- enc_wo: bfloat16 [2, 16, 128, 1024], replicated
- enc_w1: bfloat16 [2, 1024, 3072], replicated
- enc_w2: bfloat16 [2, 3072, 1024], replicated
- dec_wqkv: bfloat16 [2, 1024, 3, 16, 128], replicated
- dec_wo: bfloat16 [2, 16, 128, 1024], replicated
- cross_wq: bfloat16 [2, 1024, 8, 2, 128], replicated
- cross_wkv: bfloat16 [2, 1024, 2, 8, 128], replicated
- cross_wo: bfloat16 [2, 8, 2, 128, 1024], replicated
- dec_w1: bfloat16 [2, 1024, 3072], replicated
- dec_w2: bfloat16 [2, 3072, 1024], replicated
Outputs:
- output: bfloat16 [128, 64, 1024], P(('data', 'stage'))
All inputs are finite; a program needn't handle non-finite values.
Results may differ from the reference program's by a relative error of at most 0.0129945.
Values are sent between devices in bfloat16 or wider.
A program may use at most 1 GiB of HBM per device.

```python
import jax
import jax.numpy as jnp
from jax import lax

D = 1024
HEADS = 16
KV_HEADS = 8
HEAD = 128
FF = 3072
S_ENC = 1024
S_DEC = 64
N_SEQ = 128
L_ENC = 2
L_DEC = 2

REP = HEADS // KV_HEADS


def weight(weight_key, shape, fan_in):
    return (jax.random.normal(weight_key, shape, jnp.float32) * fan_in ** -0.5).astype(jnp.bfloat16)


def structured(key_set, length):
    trend = jnp.linspace(-1.0, 1.0, length)[None, :, None]
    common = jax.random.normal(key_set[0], (N_SEQ, 1, D), jnp.float32)
    slope = jax.random.normal(key_set[1], (N_SEQ, 1, D), jnp.float32)
    noise = jax.random.normal(key_set[2], (N_SEQ, length, D), jnp.float32)
    return (0.5 * common + 0.8 * trend * slope + 0.4 * noise).astype(jnp.bfloat16)


def setup_inputs(seed: int = 0, part: int = 0) -> dict:
    part_keys = jax.random.split(jax.random.fold_in(jax.random.key(seed), part), 7)
    weight_keys = jax.random.split(jax.random.key(seed + 1), 11)
    lengths = jax.random.randint(part_keys[6], (N_SEQ,), S_ENC // 4, S_ENC + 1, jnp.int32)
    lengths = lengths.at[0].set(S_ENC)
    return {
        "x_enc": structured(part_keys[0:3], S_ENC),
        "enc_len": lengths,
        "y": structured(part_keys[3:6], S_DEC),
        "enc_wqkv": weight(weight_keys[0], (L_ENC, D, 3, HEADS, HEAD), D),
        "enc_wo": weight(weight_keys[1], (L_ENC, HEADS, HEAD, D), HEADS * HEAD),
        "enc_w1": weight(weight_keys[2], (L_ENC, D, FF), D),
        "enc_w2": weight(weight_keys[3], (L_ENC, FF, D), FF),
        "dec_wqkv": weight(weight_keys[4], (L_DEC, D, 3, HEADS, HEAD), D),
        "dec_wo": weight(weight_keys[5], (L_DEC, HEADS, HEAD, D), HEADS * HEAD),
        "cross_wq": weight(weight_keys[6], (L_DEC, D, KV_HEADS, REP, HEAD), D),
        "cross_wkv": weight(weight_keys[7], (L_DEC, D, 2, KV_HEADS, HEAD), D),
        "cross_wo": weight(weight_keys[8], (L_DEC, KV_HEADS, REP, HEAD, D), HEADS * HEAD),
        "dec_w1": weight(weight_keys[9], (L_DEC, D, FF), D),
        "dec_w2": weight(weight_keys[10], (L_DEC, FF, D), FF),
    }


def rms_norm(inputs):
    wide = inputs.astype(jnp.float32)
    return (wide * lax.rsqrt(jnp.mean(wide * wide, axis=-1, keepdims=True) + 1e-6)).astype(jnp.bfloat16)


def attend(query, keys, values, valid):
    scores = jnp.einsum("qgrd,kgd->grqk", query.astype(jnp.float32), keys.astype(jnp.float32)) * HEAD ** -0.5
    attn_probs = jax.nn.softmax(jnp.where(valid, scores, -1e30), axis=-1).astype(jnp.bfloat16)
    return jnp.einsum("grqk,kgd->qgrd", attn_probs.astype(jnp.float32), values.astype(jnp.float32)).astype(jnp.bfloat16)


def self_block(state, w_qkv, w_out, valid):
    proj_qkv = jnp.einsum("sd,dthe->tshe", rms_norm(state).astype(jnp.float32), w_qkv.astype(jnp.float32)).astype(jnp.bfloat16)
    mixed = attend(proj_qkv[0][:, :, None, :], proj_qkv[1], proj_qkv[2], valid)
    update = jnp.einsum("shre,hev->sv", mixed.astype(jnp.float32), w_out.astype(jnp.float32))
    return (state.astype(jnp.float32) + update).astype(jnp.bfloat16)


def ffn_block(state, w_in, w_out):
    hidden = jax.nn.gelu(jnp.dot(rms_norm(state), w_in, preferred_element_type=jnp.float32)).astype(jnp.bfloat16)
    return (state.astype(jnp.float32) + jnp.dot(hidden, w_out, preferred_element_type=jnp.float32)).astype(jnp.bfloat16)


def reference(x_enc, enc_len, y, enc_wqkv, enc_wo, enc_w1, enc_w2, dec_wqkv, dec_wo, cross_wq, cross_wkv, cross_wo, dec_w1, dec_w2):
    def encode_one(pair):
        state = pair[0]
        valid = jnp.arange(S_ENC) < pair[1]
        for layer in range(L_ENC):
            state = self_block(state, enc_wqkv[layer], enc_wo[layer], valid)
            state = ffn_block(state, enc_w1[layer], enc_w2[layer])
        return rms_norm(state)

    enc_states = lax.map(encode_one, (x_enc, enc_len))
    partner_out = jnp.roll(enc_states, N_SEQ // 2, axis=0)
    partner_len = jnp.roll(enc_len, N_SEQ // 2, axis=0)
    positions = jnp.arange(S_DEC)
    causal = positions[None, :] <= positions[:, None]

    def decode_one(triple):
        state, enc_seq, length = triple
        keep = jnp.arange(S_ENC) < length
        for layer in range(L_DEC):
            state = self_block(state, dec_wqkv[layer], dec_wo[layer], causal)
            query = jnp.einsum("sd,dgre->sgre", rms_norm(state).astype(jnp.float32), cross_wq[layer].astype(jnp.float32)).astype(jnp.bfloat16)
            key_vals = jnp.einsum("sd,dtge->tsge", enc_seq.astype(jnp.float32), cross_wkv[layer].astype(jnp.float32)).astype(jnp.bfloat16)
            mixed = attend(query, key_vals[0], key_vals[1], keep)
            update = jnp.einsum("sgre,grev->sv", mixed.astype(jnp.float32), cross_wo[layer].astype(jnp.float32))
            state = (state.astype(jnp.float32) + update).astype(jnp.bfloat16)
            state = ffn_block(state, dec_w1[layer], dec_w2[layer])
        return state

    return lax.map(decode_one, (y, partner_out, partner_len))
```

```python
import jax
import jax.numpy as jnp
from jax import lax
from jax.sharding import PartitionSpec as P, NamedSharding


def rms_norm(inputs):
    wide = inputs.astype(jnp.float32)
    return (wide * lax.rsqrt(jnp.mean(wide * wide, axis=-1, keepdims=True) + 1e-6)).astype(jnp.bfloat16)


def attend(query, keys, values, valid):
    scale = query.shape[-1] ** -0.5
    scores = jnp.einsum("bqgrd,bkgd->bgrqk", query, keys, preferred_element_type=jnp.float32) * scale
    attn_probs = jax.nn.softmax(jnp.where(valid, scores, -1e30), axis=-1).astype(jnp.bfloat16)
    return jnp.einsum("bgrqk,bkgd->bqgrd", attn_probs, values, preferred_element_type=jnp.float32).astype(jnp.bfloat16)


def self_block(state, w_qkv, w_out, valid):
    proj_qkv = jnp.einsum("bsd,dthe->tbshe", rms_norm(state), w_qkv, preferred_element_type=jnp.float32).astype(jnp.bfloat16)
    mixed = attend(proj_qkv[0][:, :, :, None, :], proj_qkv[1], proj_qkv[2], valid)
    update = jnp.einsum("bshre,hev->bsv", mixed, w_out, preferred_element_type=jnp.float32)
    return (state.astype(jnp.float32) + update).astype(jnp.bfloat16)


def ffn_block(state, w_in, w_out):
    hidden = jax.nn.gelu(jnp.einsum("bsd,df->bsf", rms_norm(state), w_in, preferred_element_type=jnp.float32)).astype(jnp.bfloat16)
    update = jnp.einsum("bsf,fd->bsd", hidden, w_out, preferred_element_type=jnp.float32)
    return (state.astype(jnp.float32) + update).astype(jnp.bfloat16)


def encoder(x_enc, enc_len, enc_wqkv, enc_wo, enc_w1, enc_w2):
    valid = (jnp.arange(x_enc.shape[1])[None, :] < enc_len[:, None])[:, None, None, None, :]
    state = x_enc
    for layer in range(enc_wqkv.shape[0]):
        state = self_block(state, enc_wqkv[layer], enc_wo[layer], valid)
        state = ffn_block(state, enc_w1[layer], enc_w2[layer])
    return rms_norm(state)


def decoder(y, kv_all, kv_len, dec_wqkv, dec_wo, cross_wq, cross_wo, dec_w1, dec_w2):
    positions = jnp.arange(y.shape[1])
    causal = positions[None, :] <= positions[:, None]
    keep = (jnp.arange(kv_all.shape[3])[None, :] < kv_len[:, None])[:, None, None, None, :]
    state = y
    for layer in range(dec_wqkv.shape[0]):
        state = self_block(state, dec_wqkv[layer], dec_wo[layer], causal)
        query = jnp.einsum("bsd,dgre->bsgre", rms_norm(state), cross_wq[layer], preferred_element_type=jnp.float32).astype(jnp.bfloat16)
        mixed = attend(query, kv_all[layer, 0], kv_all[layer, 1], keep)
        update = jnp.einsum("bsgre,grev->bsv", mixed, cross_wo[layer], preferred_element_type=jnp.float32)
        state = (state.astype(jnp.float32) + update).astype(jnp.bfloat16)
        state = ffn_block(state, dec_w1[layer], dec_w2[layer])
    return state


def solution(mesh):
    stages = mesh.shape["stage"]
    swap = [(source, (source + stages // 2) % stages) for source in range(stages)]
    rows = P(("data", "stage"))
    whole = P()

    def body(x_enc, enc_len, y, enc_wqkv, enc_wo, enc_w1, enc_w2, dec_wqkv, dec_wo, cross_wq, cross_wkv, cross_wo, dec_w1, dec_w2):
        enc_out = encoder(x_enc, enc_len, enc_wqkv, enc_wo, enc_w1, enc_w2)
        kv_all = jnp.einsum("bsd,ldtge->ltbsge", enc_out, cross_wkv, preferred_element_type=jnp.float32).astype(jnp.bfloat16)
        y_recv = lax.ppermute(y, "stage", swap)
        done = decoder(y_recv, kv_all, enc_len, dec_wqkv, dec_wo, cross_wq, cross_wo, dec_w1, dec_w2)
        return lax.ppermute(done, "stage", swap)

    return jax.shard_map(body, mesh=mesh, in_specs=(rows, rows, rows) + (whole,) * 11, out_specs=rows, check_vma=False)
```

```python
import functools
import jax
import jax.numpy as jnp
from jax import lax
from jax.experimental import pallas as pl
from jax.experimental.pallas import tpu as pltpu
from jax.sharding import PartitionSpec as P

F32, BF16 = jnp.float32, jnp.bfloat16
NT = (((1,), (1,)), ((), ()))
VMEM_LIMIT = 60 * 1024 * 1024
SCORE = 128 ** -0.5 * 1.4426950408889634


def rms_norm(inputs):
    wide = inputs.astype(F32)
    return (wide * lax.rsqrt(jnp.mean(wide * wide, axis=-1, keepdims=True) + 1e-6)).astype(BF16)


def matmul(a, b):
    return jnp.dot(a, b, preferred_element_type=F32)


def heads_proj_kernel(x_ref, w_ref, o_ref, xn_ref, stage_ref):
    rows = x_ref.shape[0]

    @pl.when(pl.program_id(0) == 0)
    def _():
        for r in range(0, rows, 256):
            xn_ref[r:r + 256] = rms_norm(x_ref[r:r + 256])

    heads = w_ref.shape[3]
    for c in range(4):
        stage_ref[c] = w_ref[0, c * 256:(c + 1) * 256, 0].astype(F32).reshape(256 * heads, 128)
    for h in range(0, heads, 2):
        w = jnp.concatenate([
            jnp.concatenate([stage_ref[c, pl.ds(h + u, 256, stride=heads), :].astype(BF16) for u in range(2)], axis=1)
            for c in range(4)], axis=0)
        o_ref[0, :, h * 128:(h + 2) * 128] = matmul(xn_ref[...], w).astype(BF16)


def heads_proj(x, w, layers, parts, groups):
    n = x.shape[0]
    per = parts * groups
    count = len(layers) * per
    first = layers[0]
    return pl.pallas_call(
        heads_proj_kernel,
        grid=(count,),
        in_specs=[
            pl.BlockSpec((n, 1024), lambda j: (0, 0)),
            pl.BlockSpec((1, 1024, 1, 8, 128), lambda j: (first + j // per, 0, (j % per) // groups, j % groups, 0)),
        ],
        out_specs=pl.BlockSpec((1, n, 1024), lambda j: (j, 0, 0)),
        out_shape=jax.ShapeDtypeStruct((count, n, 1024), BF16),
        scratch_shapes=[pltpu.VMEM((n, 1024), BF16), pltpu.VMEM((4, 256 * 8, 128), F32)],
        compiler_params=pltpu.CompilerParams(vmem_limit_bytes=VMEM_LIMIT),
        name="heads_proj",
    )(x, w)


def enc_attn_kernel(len_ref, q_ref, k_ref, v_ref, o_ref, *, tq):
    n, width = q_ref.shape[1:]
    row = lax.broadcasted_iota(jnp.int32, (n, 128), 0)
    lane = lax.broadcasted_iota(jnp.int32, (n, 128), 1)
    bias = jnp.where((row >= len_ref[0]) & (lane == 0), -1e30, 0.0).astype(BF16)
    one = jnp.where(lax.broadcasted_iota(jnp.int32, (tq, 128), 1) == 0, 1.0, 0.0).astype(BF16)
    work = [(h, i) for h in range(width // 128) for i in range(n // tq)]

    def score(item):
        h, i = item
        keys = jnp.concatenate([k_ref[0, :, h * 128:(h + 1) * 128], bias], axis=1)
        query = jnp.concatenate([q_ref[0, i * tq:(i + 1) * tq, h * 128:(h + 1) * 128], one], axis=1)
        return lax.dot_general(query, keys, NT, preferred_element_type=F32)

    s = score(work[0])
    for j, (h, i) in enumerate(work):
        ahead = score(work[j + 1]) if j + 1 < len(work) else None
        top = jnp.max(s, axis=1, keepdims=True) * SCORE
        e = jnp.exp2(s * SCORE - top)
        p = (e * (1.0 / jnp.sum(e, axis=1, keepdims=True))).astype(BF16)
        o_ref[i * tq:(i + 1) * tq, h * 128:(h + 1) * 128] = matmul(p, v_ref[0, :, h * 128:(h + 1) * 128]).astype(BF16)
        s = ahead


def enc_attn(qkv, enc_len):
    n = qkv.shape[1]
    width = 256
    per = 1024 // width
    spec = lambda t: pl.BlockSpec((1, n, width), lambda j, _: (2 * t + j // per, 0, j % per))
    return pl.pallas_call(
        functools.partial(enc_attn_kernel, tq=256),
        grid_spec=pltpu.PrefetchScalarGridSpec(
            num_scalar_prefetch=1, grid=(2048 // width,),
            in_specs=[spec(0), spec(1), spec(2)],
            out_specs=pl.BlockSpec((n, width), lambda j, _: (0, j))),
        out_shape=jax.ShapeDtypeStruct((n, 2048), BF16),
        compiler_params=pltpu.CompilerParams(vmem_limit_bytes=VMEM_LIMIT),
        name="enc_attn",
    )(enc_len, qkv, qkv, qkv)


def gelu(u):
    return jax.nn.gelu(u)


def post_kernel(x_ref, mix_ref, wo_ref, w1_ref, w2_ref, o_ref, acc_ref, xn_ref, *, wo_steps, ff_steps, rb):
    step = pl.program_id(0)
    n = x_ref.shape[0]

    @pl.when(step < wo_steps)
    def _():
        for r in range(0, n, rb):
            part = matmul(mix_ref[r:r + rb], wo_ref[0])
            acc_ref[r:r + rb] = jnp.where(step == 0, x_ref[r:r + rb].astype(F32), acc_ref[r:r + rb]) + part if wo_steps > 1 else x_ref[r:r + rb].astype(F32) + part

    @pl.when(step == wo_steps - 1)
    def _():
        for r in range(0, n, rb):
            state = acc_ref[r:r + rb].astype(BF16)
            acc_ref[r:r + rb] = state.astype(F32)
            xn_ref[r:r + rb] = rms_norm(state)

    @pl.when(step >= wo_steps)
    def _():
        rows = list(range(0, n, rb))
        u = matmul(xn_ref[0:rb], w1_ref[0])
        for j, r in enumerate(rows):
            ahead = matmul(xn_ref[rows[j + 1]:rows[j + 1] + rb], w1_ref[0]) if j + 1 < len(rows) else None
            hidden = gelu(u).astype(BF16)
            acc_ref[r:r + rb] += matmul(hidden, w2_ref[0])
            u = ahead

    @pl.when(step == wo_steps + ff_steps - 1)
    def _():
        o_ref[...] = acc_ref[...].astype(BF16)


def post(x, mixed, wo, w1, w2, layer, wo_steps=1, fc=512, rb=256):
    n = x.shape[0]
    ff_steps = 3072 // fc
    kb = 2048 // wo_steps
    clip = lambda j: jnp.maximum(j - wo_steps, 0)
    return pl.pallas_call(
        functools.partial(post_kernel, wo_steps=wo_steps, ff_steps=ff_steps, rb=rb),
        grid=(wo_steps + ff_steps,),
        in_specs=[
            pl.BlockSpec((n, 1024), lambda j: (0, 0)),
            pl.BlockSpec((n, kb), lambda j: (0, jnp.minimum(j, wo_steps - 1))),
            pl.BlockSpec((1, kb, 1024), lambda j: (layer, jnp.minimum(j, wo_steps - 1), 0)),
            pl.BlockSpec((1, 1024, fc), lambda j: (layer, 0, clip(j))),
            pl.BlockSpec((1, fc, 1024), lambda j: (layer, clip(j), 0)),
        ],
        out_specs=pl.BlockSpec((n, 1024), lambda j: (0, 0)),
        out_shape=jax.ShapeDtypeStruct((n, 1024), BF16),
        scratch_shapes=[pltpu.VMEM((n, 1024), F32), pltpu.VMEM((n, 1024), BF16)],
        compiler_params=pltpu.CompilerParams(vmem_limit_bytes=VMEM_LIMIT),
        name="enc_post",
    )(x, mixed, wo, w1, w2)
def tail_kernel(len_ref, x_ref, y_ref, wkv, wqkv, wo, cq, co, w1, w2, o_ref,
                xn, stage, kvbuf, kv, bqkv, bo, bcq, bco, b1, b2, proj, mix, st, sems):
    n, m = x_ref.shape[0], y_ref.shape[0]

    def kv_copy(j):
        return pltpu.make_async_copy(wkv.at[j // 2, :, lax.rem(j, 2)], kvbuf.at[lax.rem(j, 2)], sems.at[8 + lax.rem(j, 2)])

    def layer_copies(l):
        pairs = [(wqkv.at[l, :, t], bqkv.at[t]) for t in range(3)]
        pairs += [(wo.at[l], bo), (cq.at[l], bcq), (co.at[l], bco), (w1.at[l], b1), (w2.at[l], b2)]
        return [pltpu.make_async_copy(src, dst, sems.at[i]) for i, (src, dst) in enumerate(pairs)]

    kv_copy(jnp.int32(0)).start()
    kv_copy(jnp.int32(1)).start()
    st[...] = y_ref[...]
    for r in range(0, n, 256):
        xn[r:r + 256] = rms_norm(x_ref[r:r + 256])
    for copy in layer_copies(0):
        copy.start()

    def kv_step(j, _):
        slot = lax.rem(j, 2)
        kv_copy(j).wait()
        for c in range(4):
            stage[c] = kvbuf[slot, c * 256:(c + 1) * 256].astype(F32).reshape(256 * 8, 128)

        @pl.when(j < 2)
        def _():
            kv_copy(j + 2).start()

        for h in range(0, 8, 2):
            w = jnp.concatenate([
                jnp.concatenate([stage[c, pl.ds(h + u, 256, stride=8), :].astype(BF16) for u in range(2)], axis=1)
                for c in range(4)], axis=0)
            kv[j, :, h * 128:(h + 2) * 128] = matmul(xn[...], w).astype(BF16)
        return 0

    lax.fori_loop(0, 4, kv_step, 0)

    def heads_matmul(z, buf, out):
        for half in range(2):
            for c in range(4):
                stage[c] = buf[c * 256:(c + 1) * 256, half * 8:(half + 1) * 8].astype(F32).reshape(256 * 8, 128)
            for h in range(0, 8, 2):
                w = jnp.concatenate([
                    jnp.concatenate([stage[c, pl.ds(h + u, 256, stride=8), :].astype(BF16) for u in range(2)], axis=1)
                    for c in range(4)], axis=0)
                col = half * 1024 + h * 128
                proj[out, :, col:col + 256] = matmul(z, w).astype(BF16)

    causal = lax.broadcasted_iota(jnp.int32, (m, m), 1) <= lax.broadcasted_iota(jnp.int32, (m, m), 0)
    row = lax.broadcasted_iota(jnp.int32, (n, 128), 0)
    lane = lax.broadcasted_iota(jnp.int32, (n, 128), 1)
    bias = jnp.where((row >= len_ref[0]) & (lane == 0), -1e30, 0.0).astype(BF16)
    one = jnp.where(lax.broadcasted_iota(jnp.int32, (2 * m, 128), 1) == 0, 1.0, 0.0).astype(BF16)

    def probs(s):
        top = jnp.max(s, axis=1, keepdims=True) * SCORE
        e = jnp.exp2(s * SCORE - top)
        return (e * (1.0 / jnp.sum(e, axis=1, keepdims=True))).astype(BF16)

    def layer_step(l, _):
        copies = layer_copies(l)
        after = layer_copies(1)

        def refill(i):
            @pl.when(l == 0)
            def _():
                after[i].start()

        z = rms_norm(st[...])
        for t in range(3):
            copies[t].wait()
            heads_matmul(z, bqkv.at[t], t)
            refill(t)
        for h in range(16):
            hs = slice(h * 128, (h + 1) * 128)
            s = lax.dot_general(proj[0, :, hs], proj[1, :, hs], NT, preferred_element_type=F32)
            p = probs(jnp.where(causal, s, -1e30))
            mix[:, hs] = matmul(p, proj[2, :, hs]).astype(BF16)
        copies[3].wait()
        st[...] = (st[...].astype(F32) + matmul(mix[...], bo[...])).astype(BF16)
        refill(3)
        copies[4].wait()
        heads_matmul(rms_norm(st[...]), bcq, 0)
        refill(4)
        for g in range(8):
            gs = slice(g * 128, (g + 1) * 128)
            q = jnp.concatenate([proj[0, :, (2 * g + r) * 128:(2 * g + r + 1) * 128] for r in range(2)], axis=0)
            s = lax.dot_general(jnp.concatenate([q, one], axis=1), jnp.concatenate([kv[2 * l, :, gs], bias], axis=1), NT,
                                preferred_element_type=F32)
            o = matmul(probs(s), kv[2 * l + 1, :, gs]).astype(BF16)
            for r in range(2):
                mix[:, (2 * g + r) * 128:(2 * g + r + 1) * 128] = o[r * m:(r + 1) * m]
        copies[5].wait()
        st[...] = (st[...].astype(F32) + matmul(mix[...], bco[...])).astype(BF16)
        refill(5)
        z = rms_norm(st[...])
        copies[6].wait()
        hidden = jax.nn.gelu(matmul(z, b1[...])).astype(BF16)
        refill(6)
        copies[7].wait()
        st[...] = (st[...].astype(F32) + matmul(hidden, b2[...])).astype(BF16)
        refill(7)
        return 0

    lax.fori_loop(0, 2, layer_step, 0)
    o_ref[...] = st[...]


def tail(x, enc_len, y, wkv, wqkv, wo, cq, co, w1, w2):
    n, m = x.shape[0], y.shape[0]
    vmem = pl.BlockSpec(memory_space=pltpu.VMEM)
    hbm = pl.BlockSpec(memory_space=pl.ANY)
    return pl.pallas_call(
        tail_kernel,
        in_specs=[pl.BlockSpec(memory_space=pltpu.SMEM), vmem, vmem] + [hbm] * 7,
        out_specs=vmem,
        out_shape=jax.ShapeDtypeStruct((m, 1024), BF16),
        scratch_shapes=[
            pltpu.VMEM((n, 1024), BF16), pltpu.VMEM((4, 2048, 128), F32), pltpu.VMEM((2, 1024, 8, 128), BF16),
            pltpu.VMEM((4, n, 1024), BF16),
            pltpu.VMEM((3, 1024, 16, 128), BF16), pltpu.VMEM((2048, 1024), BF16), pltpu.VMEM((1024, 16, 128), BF16),
            pltpu.VMEM((2048, 1024), BF16), pltpu.VMEM((1024, 3072), BF16), pltpu.VMEM((3072, 1024), BF16),
            pltpu.VMEM((3, m, 2048), BF16), pltpu.VMEM((m, 2048), BF16), pltpu.VMEM((m, 1024), BF16),
            pltpu.SemaphoreType.DMA((10,)),
        ],
        compiler_params=pltpu.CompilerParams(vmem_limit_bytes=66 * 1000 * 1000),
        name="decoder_tail",
    )(enc_len, x, y, wkv, wqkv, wo, cq, co, w1, w2)


def local(x_enc, enc_len, y, enc_wqkv, enc_wo, enc_w1, enc_w2, dec_wqkv, dec_wo, cross_wq, cross_wkv, cross_wo, dec_w1, dec_w2):
    state = x_enc[0]
    for layer in range(2):
        qkv = heads_proj(state, enc_wqkv, (layer,), 3, 2)
        mixed = enc_attn(qkv, enc_len)
        state = post(state, mixed, enc_wo.reshape(2, 2048, 1024), enc_w1, enc_w2, layer, 2, 768, 256)
    return tail(state, enc_len, y[0], cross_wkv, dec_wqkv, dec_wo.reshape(2, 2048, 1024),
                cross_wq.reshape(2, 1024, 16, 128), cross_wo.reshape(2, 2048, 1024), dec_w1, dec_w2)[None]


def solution(mesh):
    stages = mesh.shape["stage"]
    swap = [(source, (source + stages // 2) % stages) for source in range(stages)]
    rows = P(("data", "stage"))
    whole = P()

    def body(x_enc, enc_len, y, *weights):
        done = local(x_enc, enc_len, lax.ppermute(y, "stage", swap), *weights)
        return lax.ppermute(done, "stage", swap)

    return jax.shard_map(body, mesh=mesh, in_specs=(rows, rows, rows) + (whole,) * 11, out_specs=rows, check_vma=False)
```

```python
import jax
import jax.numpy as jnp
from jax import lax
from jax.experimental import pallas as pl
from jax.experimental.pallas import tpu as pltpu
from jax.sharding import PartitionSpec as P

F32, BF16 = jnp.float32, jnp.bfloat16
NT = (((1,), (1,)), ((), ()))
SCORE = 128 ** -0.5 * 1.4426950408889634
TQ = 256
RB = 256
FC = 1024


def rms_norm(inputs):
    wide = inputs.astype(F32)
    return (wide * lax.rsqrt(jnp.mean(wide * wide, axis=-1, keepdims=True) + 1e-6)).astype(BF16)


def matmul(a, b):
    return jnp.dot(a, b, preferred_element_type=F32)


def probs(s):
    top = jnp.max(s, axis=1, keepdims=True) * SCORE
    e = jnp.exp2(s * SCORE - top)
    return (e * (1.0 / jnp.sum(e, axis=1, keepdims=True))).astype(BF16)


def project8(z_ref, w_ref, half, stage, write):
    rows = pl.ds(pl.multiple_of(half * 8, 8), 8)
    for c in range(4):
        stage[c] = w_ref[c * 256:(c + 1) * 256, rows, :].astype(F32).reshape(256 * 8, 128)
    for h in range(0, 8, 2):
        w = jnp.concatenate([
            jnp.concatenate([stage[c, pl.ds(h + u, 256, stride=8), :].astype(BF16) for u in range(2)], axis=1)
            for c in range(4)], axis=0)
        write(h * 128, matmul(z_ref[...], w).astype(BF16))


def row_kernel(len_ref, y_ref, x, e_qkv, e_o, e_1, e_2, d_qkv, d_o, c_q, c_kv, c_o, d_1, d_2, o_ref,
               state, xn, qkv, stage, b_qkv, b_o, b_cq, b_co, b_1, b_2, proj, mix, st, z, sems):
    n, m = state.shape[0], y_ref.shape[0]
    enc, dec = (e_qkv, e_o, e_1, e_2), (d_qkv, d_o, d_1, d_2)

    def copy(which, l, i):
        src = which[0].at[l, :, i] if not isinstance(i, int) or i < 3 else which[i - 2].at[l]
        dst = b_qkv.at[i] if not isinstance(i, int) or i < 3 else (b_o, b_1, b_2)[i - 3]
        return pltpu.make_async_copy(src, dst, sems.at[i])

    def co_copy(l):
        return pltpu.make_async_copy(c_o.at[l], b_co, sems.at[6])

    def cq_copy(l):
        return pltpu.make_async_copy(c_q.at[l], b_cq, sems.at[7])

    def kv_copy(j):
        slot = lax.rem(j, 2)
        return pltpu.make_async_copy(c_kv.at[j // 2, :, lax.rem(j, 2)],
                                     b_cq.at[:, pl.ds(pl.multiple_of(slot * 8, 8), 8)], sems.at[8 + slot])

    x_copy = pltpu.make_async_copy(x, state, sems.at[10])
    x_copy.start()
    for i in range(3):
        copy(enc, 0, i).start()
    st[...] = y_ref[...]
    row = lax.broadcasted_iota(jnp.int32, (n, 128), 0)
    lane = lax.broadcasted_iota(jnp.int32, (n, 128), 1)
    bias = jnp.where((row >= len_ref[0]) & (lane == 0), -1e30, 0.0).astype(BF16)
    one = jnp.where(lax.broadcasted_iota(jnp.int32, (TQ, 128), 1) == 0, 1.0, 0.0).astype(BF16)
    x_copy.wait()
    for r in range(0, n, RB):
        xn[r:r + RB] = rms_norm(state[r:r + RB])
    for i in range(3, 6):
        copy(enc, 0, i).start()
    co_copy(0).start()
    kv_copy(jnp.int32(0)).start()
    kv_copy(jnp.int32(1)).start()

    def enc_layer(l, _):
        def refill(i):
            @pl.when(l == 0)
            def _():
                copy(enc, 1, i).start()

            @pl.when(l == 1)
            def _():
                copy(dec, 0, i).start()

        def qkv_step(j, _):
            t, half = j // 2, lax.rem(j, 2)

            @pl.when(half == 0)
            def _():
                copy(enc, 0, t).wait()

            def write(col, value):
                qkv[j, :, col:col + 256] = value

            project8(xn, b_qkv.at[t], half, stage, write)

            @pl.when(half == 1)
            def _():
                refill(t)

            return 0

        lax.fori_loop(0, 6, qkv_step, 0)

        def attn_step(j, _):
            half, base = j // 4, lax.rem(j, 4) * 256
            work = [(h, i) for h in range(2) for i in range(n // TQ)]

            def cols(h):
                return pl.ds(pl.multiple_of(base + h * 128, 128), 128)

            def score(item):
                h, i = item
                keys = jnp.concatenate([qkv[2 + half, :, cols(h)], bias], axis=1)
                query = jnp.concatenate([qkv[half, i * TQ:(i + 1) * TQ, cols(h)], one], axis=1)
                return lax.dot_general(query, keys, NT, preferred_element_type=F32)

            s = score(work[0])
            for k, (h, i) in enumerate(work):
                ahead = score(work[k + 1]) if k + 1 < len(work) else None
                qkv[half, i * TQ:(i + 1) * TQ, cols(h)] = matmul(probs(s), qkv[4 + half, :, cols(h)]).astype(BF16)
                s = ahead
            return 0

        lax.fori_loop(0, 8, attn_step, 0)

        for i in range(3, 6):
            copy(enc, 0, i).wait()

        def ffn_step(j, _):
            rs = pl.ds(pl.multiple_of(j * RB, RB), RB)
            mixed = jnp.concatenate([qkv[0, rs, :], qkv[1, rs, :]], axis=1)
            mid = (state[rs, :].astype(F32) + matmul(mixed, b_o[...])).astype(BF16)
            normed = rms_norm(mid)
            total = mid.astype(F32)
            u = matmul(normed, b_1[:, 0:FC])
            for c in range(0, 3072, FC):
                ahead = matmul(normed, b_1[:, c + FC:c + 2 * FC]) if c + FC < 3072 else None
                total += matmul(jax.nn.gelu(u).astype(BF16), b_2[c:c + FC, :])
                u = ahead
            done = total.astype(BF16)
            state[rs, :] = done
            xn[rs, :] = rms_norm(done)
            return 0

        lax.fori_loop(0, n // RB, ffn_step, 0)
        for i in range(3, 6):
            refill(i)
        return 0

    lax.fori_loop(0, 2, enc_layer, 0)

    def kv_step(j, _):
        kv_copy(j).wait()

        def write(col, value):
            qkv[j, :, col:col + 256] = value

        project8(xn, b_cq, lax.rem(j, 2), stage, write)

        @pl.when(j < 2)
        def _():
            kv_copy(j + 2).start()

        return 0

    lax.fori_loop(0, 4, kv_step, 0)
    cq_copy(0).start()

    causal = lax.broadcasted_iota(jnp.int32, (m, m), 1) <= lax.broadcasted_iota(jnp.int32, (m, m), 0)
    causal = jnp.concatenate([causal] * 16, axis=0)

    def dec_layer(l, _):
        def again(start):
            @pl.when(l == 0)
            def _():
                start()

        z[...] = rms_norm(st[...])

        def qkv_step(j, _):
            t, half = j // 2, lax.rem(j, 2)

            @pl.when(half == 0)
            def _():
                copy(dec, 0, t).wait()

            def write(col, value):
                proj[t, :, pl.ds(pl.multiple_of(half * 1024 + col, 256), 256)] = value

            project8(z, b_qkv.at[t], half, stage, write)

            @pl.when((half == 1) & (l == 0))
            def _():
                copy(dec, 1, t).start()

            return 0

        lax.fori_loop(0, 6, qkv_step, 0)
        heads = [slice(h * 128, (h + 1) * 128) for h in range(16)]
        s = [lax.dot_general(proj[0, :, hs], proj[1, :, hs], NT, preferred_element_type=F32) for hs in heads]
        p = probs(jnp.where(causal, jnp.concatenate(s, axis=0), -1e30))
        o = [matmul(p[i * m:(i + 1) * m], proj[2, :, hs]) for i, hs in enumerate(heads)]
        mix[...] = jnp.concatenate(o, axis=1).astype(BF16)
        copy(dec, 0, 3).wait()
        st[...] = (st[...].astype(F32) + matmul(mix[...], b_o[...])).astype(BF16)
        again(lambda: copy(dec, 1, 3).start())
        z[...] = rms_norm(st[...])
        cq_copy(0).wait()

        def cq_step(half, _):
            def write(col, value):
                proj[0, :, pl.ds(pl.multiple_of(half * 1024 + col, 256), 256)] = value

            project8(z, b_cq, half, stage, write)
            return 0

        lax.fori_loop(0, 2, cq_step, 0)
        again(lambda: cq_copy(1).start())
        for base in (0, 4):
            s = []
            for g in range(base, base + 4):
                q = jnp.concatenate([proj[0, :, heads[2 * g + r]] for r in range(2)], axis=0)
                s.append(lax.dot_general(jnp.concatenate([q, one[:2 * m]], axis=1),
                                         jnp.concatenate([qkv[2 * l, :, heads[g]], bias], axis=1), NT,
                                         preferred_element_type=F32))
            p = [probs(part) for part in s]
            for i in range(4):
                g = base + i
                o = matmul(p[i], qkv[2 * l + 1, :, heads[g]]).astype(BF16)
                for r in range(2):
                    mix[:, heads[2 * g + r]] = o[r * m:(r + 1) * m]
        co_copy(0).wait()
        st[...] = (st[...].astype(F32) + matmul(mix[...], b_co[...])).astype(BF16)
        again(lambda: co_copy(1).start())
        copy(dec, 0, 4).wait()
        hidden = jax.nn.gelu(matmul(rms_norm(st[...]), b_1[...])).astype(BF16)
        again(lambda: copy(dec, 1, 4).start())
        copy(dec, 0, 5).wait()
        st[...] = (st[...].astype(F32) + matmul(hidden, b_2[...])).astype(BF16)
        again(lambda: copy(dec, 1, 5).start())
        return 0

    lax.fori_loop(0, 2, dec_layer, 0)
    o_ref[...] = st[...]


def local(x_enc, enc_len, y, enc_wqkv, enc_wo, enc_w1, enc_w2, dec_wqkv, dec_wo, cross_wq, cross_wkv, cross_wo, dec_w1, dec_w2):
    n, m = x_enc.shape[1], y.shape[1]
    vmem = pl.BlockSpec(memory_space=pltpu.VMEM)
    flat = lambda w: w.reshape(2, 2048, 1024)
    return pl.pallas_call(
        row_kernel,
        in_specs=[pl.BlockSpec(memory_space=pltpu.SMEM), vmem] + [pl.BlockSpec(memory_space=pl.ANY)] * 12,
        out_specs=vmem,
        out_shape=jax.ShapeDtypeStruct((m, 1024), BF16),
        scratch_shapes=[
            pltpu.VMEM((n, 1024), BF16), pltpu.VMEM((n, 1024), BF16), pltpu.VMEM((6, n, 1024), BF16),
            pltpu.VMEM((4, 2048, 128), F32), pltpu.VMEM((3, 1024, 16, 128), BF16), pltpu.VMEM((2048, 1024), BF16),
            pltpu.VMEM((1024, 16, 128), BF16), pltpu.VMEM((2048, 1024), BF16),
            pltpu.VMEM((1024, 3072), BF16), pltpu.VMEM((3072, 1024), BF16),
            pltpu.VMEM((3, m, 2048), BF16), pltpu.VMEM((m, 2048), BF16), pltpu.VMEM((m, 1024), BF16),
            pltpu.VMEM((m, 1024), BF16), pltpu.SemaphoreType.DMA((11,)),
        ],
        compiler_params=pltpu.CompilerParams(vmem_limit_bytes=67_000_000),
        name="row",
    )(enc_len, y[0], x_enc[0], enc_wqkv, flat(enc_wo), enc_w1, enc_w2, dec_wqkv, flat(dec_wo),
      cross_wq.reshape(2, 1024, 16, 128), cross_wkv, flat(cross_wo), dec_w1, dec_w2)[None]


def solution(mesh):
    stages = mesh.shape["stage"]
    swap = [(source, (source + stages // 2) % stages) for source in range(stages)]
    rows = P(("data", "stage"))
    whole = P()

    def body(x_enc, enc_len, y, *weights):
        done = local(x_enc, enc_len, lax.ppermute(y, "stage", swap), *weights)
        return lax.ppermute(done, "stage", swap)

    return jax.shard_map(body, mesh=mesh, in_specs=(rows, rows, rows) + (whole,) * 11, out_specs=rows, check_vma=False)
```

```python
import jax
import jax.numpy as jnp
from jax import lax
from jax.experimental import pallas as pl
from jax.experimental.pallas import tpu as pltpu
from jax.sharding import PartitionSpec as P

F32, BF16 = jnp.float32, jnp.bfloat16
NT = (((1,), (1,)), ((), ()))
SCORE = 128 ** -0.5 * 1.4426950408889634
TQ = 256
RB = 256
FC = 1024


def rms_norm(inputs):
    wide = inputs.astype(F32)
    return (wide * lax.rsqrt(jnp.mean(wide * wide, axis=-1, keepdims=True) + 1e-6)).astype(BF16)


def matmul(a, b):
    return jnp.dot(a, b, preferred_element_type=F32)


def probs(s):
    top = jnp.max(s, axis=1, keepdims=True) * SCORE
    e = jnp.exp2(s * SCORE - top)
    return (e * (1.0 / jnp.sum(e, axis=1, keepdims=True))).astype(BF16)


def project8(z_ref, w_ref, half, stage, write):
    rows = pl.ds(pl.multiple_of(half * 8, 8), 8)
    for c in range(4):
        stage[c] = w_ref[c * 256:(c + 1) * 256, rows, :].astype(F32).reshape(256 * 8, 128)
    for h in range(0, 8, 2):
        w = jnp.concatenate([
            jnp.concatenate([stage[c, pl.ds(h + u, 256, stride=8), :].astype(BF16) for u in range(2)], axis=1)
            for c in range(4)], axis=0)
        write(h * 128, matmul(z_ref[...], w).astype(BF16))


def project16(z, w_ref, stage, write):
    def fill(k):
        c, rows = k % 4, slice(k // 4 * 8, k // 4 * 8 + 8)
        stage[c] = w_ref[c * 256:(c + 1) * 256, rows, :].astype(F32).reshape(256 * 8, 128)

    fill(0)
    fill(1)
    total = {}
    for k in range(8):
        if k + 2 < 8:
            fill(k + 2)
        c = k % 4
        for h in range(0, 8, 2):
            w = jnp.concatenate([stage[c, pl.ds(h + u, 256, stride=8), :].astype(BF16) for u in range(2)], axis=1)
            part = matmul(z[:, c * 256:(c + 1) * 256], w)
            total[h] = part if c == 0 else total[h] + part
        if c == 3:
            for h in range(0, 8, 2):
                write(k // 4 * 1024 + h * 128, total[h].astype(BF16))


def row_kernel(len_ref, y_ref, x, e_qkv, e_o, e_1, e_2, d_qkv, d_o, c_q, c_kv, c_o, d_1, d_2, o_ref,
               state, xn, qkv, stage, b_qkv, b_o, b_cq, b_co, b_1, b_2, pair, proj, mix, st, z, sems):
    n, m = state.shape[0], y_ref.shape[0]
    enc, dec = (e_qkv, e_o, e_1, e_2), (d_qkv, d_o, d_1, d_2)

    def copy(which, l, i):
        src = which[0].at[l, :, i] if not isinstance(i, int) or i < 3 else which[i - 2].at[l]
        dst = b_qkv.at[i] if not isinstance(i, int) or i < 3 else (b_o, b_1, b_2)[i - 3]
        return pltpu.make_async_copy(src, dst, sems.at[i])

    def co_copy(l):
        return pltpu.make_async_copy(c_o.at[l], b_co, sems.at[6])

    def cq_copy(l):
        return pltpu.make_async_copy(c_q.at[l], b_cq, sems.at[7])

    def kv_copy(j):
        slot = lax.rem(j, 2)
        return pltpu.make_async_copy(c_kv.at[j // 2, :, lax.rem(j, 2)],
                                     b_cq.at[:, pl.ds(pl.multiple_of(slot * 8, 8), 8)], sems.at[8 + slot])

    x_copy = pltpu.make_async_copy(x, state, sems.at[10])
    x_copy.start()
    for i in range(3):
        copy(enc, 0, i).start()
    st[...] = y_ref[...]
    row = lax.broadcasted_iota(jnp.int32, (n, 128), 0)
    lane = lax.broadcasted_iota(jnp.int32, (n, 128), 1)
    bias = jnp.where((row >= len_ref[0]) & (lane == 0), -1e30, 0.0).astype(BF16)
    one = jnp.where(lax.broadcasted_iota(jnp.int32, (TQ, 128), 1) == 0, 1.0, 0.0).astype(BF16)
    x_copy.wait()
    for r in range(0, n, RB):
        xn[r:r + RB] = rms_norm(state[r:r + RB])
    for i in range(3, 6):
        copy(enc, 0, i).start()
    co_copy(0).start()
    kv_copy(jnp.int32(0)).start()
    kv_copy(jnp.int32(1)).start()

    def enc_layer(l, _):
        def refill(i):
            @pl.when(l == 0)
            def _():
                copy(enc, 1, i).start()

            @pl.when(l == 1)
            def _():
                copy(dec, 0, i).start()

        def qkv_step(j, _):
            t, half = j // 2, lax.rem(j, 2)

            @pl.when(half == 0)
            def _():
                copy(enc, 0, t).wait()

            def write(col, value):
                qkv[j * 4 + col // 256] = value

            project8(xn, b_qkv.at[t], half, stage, write)

            @pl.when(half == 1)
            def _():
                refill(t)

            return 0

        lax.fori_loop(0, 6, qkv_step, 0)

        def attn_step(j, _):
            work = [(h, i) for h in range(4) for i in range(n // TQ)]

            def block(h):
                return 2 * j + h // 2

            def cols(h):
                return slice(h % 2 * 128, (h % 2 + 1) * 128)

            def score(item):
                h, i = item
                keys = jnp.concatenate([qkv[8 + block(h), :, cols(h)], bias], axis=1)
                query = jnp.concatenate([qkv[block(h), i * TQ:(i + 1) * TQ, cols(h)], one], axis=1)
                return lax.dot_general(query, keys, NT, preferred_element_type=F32)

            s = score(work[0])
            for k, (h, i) in enumerate(work):
                ahead = score(work[k + 1]) if k + 1 < len(work) else None
                pair[h // 2, i * TQ:(i + 1) * TQ, cols(h)] = matmul(probs(s), qkv[16 + block(h), :, cols(h)]).astype(BF16)
                s = ahead
            for b in range(2):
                qkv[2 * j + b] = pair[b]
            return 0

        lax.fori_loop(0, 4, attn_step, 0)

        for i in range(3, 6):
            copy(enc, 0, i).wait()

        def ffn_step(j, _):
            rs = pl.ds(pl.multiple_of(j * RB, RB), RB)
            mixed = jnp.concatenate([qkv[c, rs, :] for c in range(8)], axis=1)
            mid = (state[rs, :].astype(F32) + matmul(mixed, b_o[...])).astype(BF16)
            normed = rms_norm(mid)
            total = mid.astype(F32)
            u = matmul(normed, b_1[:, 0:FC])
            for c in range(0, 3072, FC):
                ahead = matmul(normed, b_1[:, c + FC:c + 2 * FC]) if c + FC < 3072 else None
                total += matmul(jax.nn.gelu(u).astype(BF16), b_2[c:c + FC, :])
                u = ahead
            done = total.astype(BF16)
            state[rs, :] = done
            xn[rs, :] = rms_norm(done)
            return 0

        lax.fori_loop(0, n // RB, ffn_step, 0)
        for i in range(3, 6):
            refill(i)
        return 0

    lax.fori_loop(0, 2, enc_layer, 0)

    def kv_step(j, _):
        kv_copy(j).wait()

        def write(col, value):
            qkv[j * 4 + col // 256] = value

        project8(xn, b_cq, lax.rem(j, 2), stage, write)

        @pl.when(j < 2)
        def _():
            kv_copy(j + 2).start()

        return 0

    lax.fori_loop(0, 4, kv_step, 0)
    cq_copy(0).start()

    causal = lax.broadcasted_iota(jnp.int32, (m, m), 1) <= lax.broadcasted_iota(jnp.int32, (m, m), 0)
    causal = jnp.concatenate([causal] * 16, axis=0)

    def dec_layer(l, _):
        def again(start):
            @pl.when(l == 0)
            def _():
                start()

        z[...] = rms_norm(st[...])

        def qkv_step(t, _):
            copy(dec, 0, t).wait()

            def write(col, value):
                proj[t, :, col:col + 256] = value

            project16(z[...], b_qkv.at[t], stage, write)
            again(lambda: copy(dec, 1, t).start())
            return 0

        lax.fori_loop(0, 3, qkv_step, 0)
        heads = [slice(h * 128, (h + 1) * 128) for h in range(16)]
        s = [lax.dot_general(proj[0, :, hs], proj[1, :, hs], NT, preferred_element_type=F32) for hs in heads]
        p = probs(jnp.where(causal, jnp.concatenate(s, axis=0), -1e30))
        o = [matmul(p[i * m:(i + 1) * m], proj[2, :, hs]) for i, hs in enumerate(heads)]
        mix[...] = jnp.concatenate(o, axis=1).astype(BF16)
        copy(dec, 0, 3).wait()
        st[...] = (st[...].astype(F32) + matmul(mix[...], b_o[...])).astype(BF16)
        again(lambda: copy(dec, 1, 3).start())
        z[...] = rms_norm(st[...])
        cq_copy(0).wait()

        def write(col, value):
            proj[0, :, col:col + 256] = value

        project16(z[...], b_cq, stage, write)
        again(lambda: cq_copy(1).start())
        for base in (0, 4):
            s = []
            for g in range(base, base + 4):
                q = jnp.concatenate([proj[0, :, heads[2 * g + r]] for r in range(2)], axis=0)
                s.append(lax.dot_general(jnp.concatenate([q, one[:2 * m]], axis=1),
                                         jnp.concatenate([qkv[8 * l + g // 2, :, heads[g % 2]], bias], axis=1), NT,
                                         preferred_element_type=F32))
            p = [probs(part) for part in s]
            for i in range(4):
                g = base + i
                o = matmul(p[i], qkv[8 * l + 4 + g // 2, :, heads[g % 2]]).astype(BF16)
                for r in range(2):
                    mix[:, heads[2 * g + r]] = o[r * m:(r + 1) * m]
        co_copy(0).wait()
        st[...] = (st[...].astype(F32) + matmul(mix[...], b_co[...])).astype(BF16)
        again(lambda: co_copy(1).start())
        copy(dec, 0, 4).wait()
        hidden = jax.nn.gelu(matmul(rms_norm(st[...]), b_1[...])).astype(BF16)
        again(lambda: copy(dec, 1, 4).start())
        copy(dec, 0, 5).wait()
        st[...] = (st[...].astype(F32) + matmul(hidden, b_2[...])).astype(BF16)
        again(lambda: copy(dec, 1, 5).start())
        return 0

    lax.fori_loop(0, 2, dec_layer, 0)
    o_ref[...] = st[...]


def local(x_enc, enc_len, y, enc_wqkv, enc_wo, enc_w1, enc_w2, dec_wqkv, dec_wo, cross_wq, cross_wkv, cross_wo, dec_w1, dec_w2):
    n, m = x_enc.shape[1], y.shape[1]
    vmem = pl.BlockSpec(memory_space=pltpu.VMEM)
    flat = lambda w: w.reshape(2, 2048, 1024)
    return pl.pallas_call(
        row_kernel,
        in_specs=[pl.BlockSpec(memory_space=pltpu.SMEM), vmem] + [pl.BlockSpec(memory_space=pl.ANY)] * 12,
        out_specs=vmem,
        out_shape=jax.ShapeDtypeStruct((m, 1024), BF16),
        scratch_shapes=[
            pltpu.VMEM((n, 1024), BF16), pltpu.VMEM((n, 1024), BF16), pltpu.VMEM((24, n, 256), BF16),
            pltpu.VMEM((4, 2048, 128), F32), pltpu.VMEM((3, 1024, 16, 128), BF16), pltpu.VMEM((2048, 1024), BF16),
            pltpu.VMEM((1024, 16, 128), BF16), pltpu.VMEM((2048, 1024), BF16),
            pltpu.VMEM((1024, 3072), BF16), pltpu.VMEM((3072, 1024), BF16),
            pltpu.VMEM((2, n, 256), BF16), pltpu.VMEM((3, m, 2048), BF16), pltpu.VMEM((m, 2048), BF16), pltpu.VMEM((m, 1024), BF16),
            pltpu.VMEM((m, 1024), BF16), pltpu.SemaphoreType.DMA((11,)),
        ],
        compiler_params=pltpu.CompilerParams(vmem_limit_bytes=67_000_000),
        name="row",
    )(enc_len, y[0], x_enc[0], enc_wqkv, flat(enc_wo), enc_w1, enc_w2, dec_wqkv, flat(dec_wo),
      cross_wq.reshape(2, 1024, 16, 128), cross_wkv, flat(cross_wo), dec_w1, dec_w2)[None]


def solution(mesh):
    stages = mesh.shape["stage"]
    swap = [(source, (source + stages // 2) % stages) for source in range(stages)]
    rows = P(("data", "stage"))
    whole = P()

    def body(x_enc, enc_len, y, *weights):
        done = local(x_enc, enc_len, lax.ppermute(y, "stage", swap), *weights)
        return lax.ppermute(done, "stage", swap)

    return jax.shard_map(body, mesh=mesh, in_specs=(rows, rows, rows) + (whole,) * 11, out_specs=rows, check_vma=False)
```
